32 devices in a mesh: gx: 4 (over z), gy: 8 (over y, x, core).
Axes of the slice: x: 2, y: 2, z: 4, core: 2. Of those that a mesh axis runs over, the one named last changes fastest.
Arguments:
- greens: bfloat16 [32, 125, 250], P('gy'), may hold values from -6 to 7
- chol_rot: bfloat16 [896, 125, 250], P(('gx', 'gy')), may hold values from -0.0024414062 to 0.0024414062
- one_body: float32 [125, 250], replicated, may hold values from -1 to 1
- weights: float32 [32], P('gy'), may hold values from 0.1 to 10
Outputs:
- local_energy: float32 [32], P('gy')
- mean_energy: float32 [], replicated
The draws below stay inside these ranges and needn't reach their ends.
All inputs are finite; a program needn't handle non-finite values.
Results may differ from the reference program's by a relative error of at most 0.0003.
Values may be sent and summed in bfloat16 or wider, within the bound.
A program may use at most 256 MiB of HBM per device.

```python
import math
import jax
import jax.numpy as jnp
from jax import lax

NORB = 250
NOCC = 125
NCHOL = 896
WALKERS = 32


def occupied_block():
    rows = jnp.arange(NOCC)[:, None]
    cols = jnp.arange(NORB)[None, :]
    return (rows == cols).astype(jnp.float32)


def draw_greens(key, part):
    noise_key = jax.random.fold_in(key, 11)
    noise = jax.random.normal(noise_key, (WALKERS, NOCC, NORB), jnp.float32)
    noise = jnp.clip(noise, -6.0, 6.0)
    return (occupied_block()[None, :, :] + noise).astype(jnp.bfloat16)


def draw_one_body(key, part):
    noise_key = jax.random.fold_in(key, 21)
    spread = (NOCC * NORB) ** (-0.5)
    noise = jnp.clip(jax.random.normal(noise_key, (NOCC, NORB), jnp.float32), -6.0, 6.0) * spread
    return (noise - 4.0 / NOCC * occupied_block()).astype(jnp.float32)


def block_scale(key, extent, cuts, low, high):
    loudness = 1.0
    for axis_at, blocks in cuts:
        steps = jax.random.uniform(jax.random.fold_in(jax.random.fold_in(key, 6), axis_at), (blocks,), jnp.float32, low / len(cuts), high / len(cuts))
        loudness = loudness * jnp.repeat(jnp.exp(steps), extent[axis_at] // blocks).reshape((-1,) + (1,) * (len(extent) - 1 - axis_at))
    return loudness


def gaussian(key, extent, width, reach, shards=(), kind=jnp.bfloat16):
    values = width * jax.random.normal(key, extent, jnp.float32)
    if shards:
        values = values * block_scale(key, extent, shards, -0.22, 0.18)
    return jnp.clip(values, -reach, reach).astype(kind)


def setup_inputs(seed: int = 0) -> dict:
    seeds = jax.random.split(jax.random.key(seed), 5)
    return {
        "greens": draw_greens(jax.random.fold_in(seeds[4], 71), 0),
        "chol_rot": gaussian(seeds[1], (NCHOL, NOCC, NORB), (NCHOL * NOCC * NORB // 4) ** -0.5, 0.0024414062, ((0, 32),)),
        "one_body": draw_one_body(jax.random.fold_in(seeds[4], 71), 0),
        "weights": jnp.clip(jnp.exp(math.log(10.0) - 4.6051702 * jax.random.uniform(seeds[3], (WALKERS,), jnp.float32) ** block_scale(seeds[3], (WALKERS,), ((0, 8),), -0.2, 0.2)), 0.1, 10.0),
    }


def pair_energy(green_block, vector_block):
    walkers = green_block.shape[0]
    vectors = vector_block.shape[0]
    occ = green_block.shape[1]
    orb = green_block.shape[2]
    coulomb = jnp.dot(green_block.reshape(walkers, occ * orb), vector_block.reshape(vectors, occ * orb).T, preferred_element_type=jnp.float32)
    exchange = jnp.dot(green_block.reshape(walkers * occ, orb), vector_block.reshape(vectors * occ, orb).T, preferred_element_type=jnp.float32)
    exchange = exchange.reshape(walkers, occ, vectors, occ)
    swapped = jnp.transpose(exchange, (0, 3, 2, 1))
    return 0.5 * jnp.sum(coulomb * coulomb, axis=1) - 0.5 * jnp.sum(exchange * swapped, axis=(1, 2, 3))


def reference(greens, chol_rot, one_body, weights):
    block = math.gcd(NCHOL, 16)
    stacked = chol_rot.reshape(NCHOL // block, block, NOCC, NORB)

    def step(total, vector_block):
        return total + pair_energy(greens, vector_block), None

    two_body, unused = lax.scan(step, jnp.zeros((WALKERS,), jnp.float32), stacked)
    single = jnp.sum(greens.astype(jnp.float32) * one_body[None, :, :], axis=(1, 2))
    local_energy = single + two_body
    mean_energy = jnp.sum(weights * local_energy) / jnp.sum(weights)
    return local_energy, mean_energy
```

```python
import functools

import jax
import jax.numpy as jnp
from jax import lax
from jax.experimental import pallas as pl
from jax.experimental.pallas import tpu as pltpu
from jax.sharding import PartitionSpec as P

MESH = pl.DeviceIdType.MESH
LANE = 128


def up(value, unit):
    return -(-value // unit) * unit


def bits_of(mask):
    return [1 << b for b in range(mask.bit_length()) if mask >> b & 1]


def last_hop(mask, half):
    if mask & 1:
        return 1
    found = bits_of(mask)
    return found[-1] if half == 0 else found[0]


def depth_of(mask):
    return 2 * len(bits_of(mask & ~1)) + (mask & 1)


def arrival_steps(peers, halves):
    units = [(mask, half) for mask in range(peers) for half in range(halves)]
    if halves == 1:
        return [[unit] for unit in sorted(units, key=lambda u: (depth_of(u[0]), u[0]))]

    def rank(unit):
        mask, half = unit
        rest = mask & ~1
        late = 0
        if len(bits_of(rest)) == 1:
            late = (half + bits_of(rest)[0].bit_length()) % 2
        return (depth_of(mask), late, mask, half)

    units.sort(key=rank)
    return [units[i:i + 2] for i in range(0, len(units), 2)]


def kernel(ngx, ngy, greens_ref, chol_ref, body_ref, weight_ref, energy_ref, mean_ref,
           slots, gz, lp, lt, dga, dgb, rows, part, box_x, box_y, msg_x, msg_y,
           send_sem, recv_sem, xs_sem, xr_sem, ys_sem, yr_sem):
    gx = lax.axis_index("gx")
    gy = lax.axis_index("gy")
    wl, occ, orb = greens_ref.shape
    ng = chol_ref.shape[0]
    occ_p = lp.shape[0]
    tiles = lt.shape[1] // (2 * occ_p)
    halves = 2 if wl % 2 == 0 else 1
    hw = wl // halves

    def flip(mask):
        there = gy
        for bit in bits_of(mask):
            there = there + bit * (1 - 2 * ((there // bit) % 2))
        return there

    def x_peer(step):
        return (gx + step) % ngx

    barrier = pltpu.get_barrier_semaphore()
    for mask in range(1, ngy):
        pl.semaphore_signal(barrier, inc=1, device_id=(gx, flip(mask)), device_id_type=MESH)
    for step in range(1, ngx):
        pl.semaphore_signal(barrier, inc=1, device_id=(x_peer(step), gy), device_id_type=MESH)
    pl.semaphore_wait(barrier, ngy - 1 + ngx - 1)

    def hop(mask, half):
        over = last_hop(mask, half)
        before = mask ^ over
        span = pl.ds(half * hw, hw)
        source = greens_ref.at[span] if before == 0 else slots.at[before, span]
        return pltpu.make_async_remote_copy(
            src_ref=source, dst_ref=slots.at[mask, span],
            send_sem=send_sem.at[mask, half], recv_sem=recv_sem.at[mask, half],
            device_id=(gx, flip(over)), device_id_type=MESH)

    steps = arrival_steps(ngy, halves)
    order = [unit for step in steps for unit in step]

    def forward(unit):
        for mask, half in order:
            if mask and half == unit[1] and mask ^ last_hop(mask, half) == unit[0]:
                hop(mask, half).start()

    for half in range(halves):
        forward((0, half))

    gz[...] = jnp.zeros_like(gz)
    lp[...] = jnp.zeros_like(lp)
    for g in range(2 * tiles):
        if g < ng:
            lp[0:occ, 0:orb] = chol_ref[g]
            lt[:, g * occ_p:(g + 1) * occ_p] = lp[...].T
        else:
            lt[:, g * occ_p:(g + 1) * occ_p] = jnp.zeros((lt.shape[0], occ_p), lt.dtype)

    lane8 = lax.broadcasted_iota(jnp.int32, (8, occ_p), 1)
    sub8 = lax.broadcasted_iota(jnp.int32, (8, occ_p), 0)
    on_diag = (lane8 % 8) == sub8
    below = (lax.broadcasted_iota(jnp.int32, (occ_p, occ_p), 0)
             > lax.broadcasted_iota(jnp.int32, (occ_p, occ_p), 1))

    def diagonal(block):
        picked = block[0:8]
        for k in range(1, occ_p // 8):
            picked = jnp.where(lane8 >= 8 * k, block[8 * k:8 * k + 8], picked)
        return jnp.sum(jnp.where(on_diag, picked, 0.0), axis=0, keepdims=True)

    def step_body(s, carry):
        for at, units in enumerate(steps):
            @pl.when(s == at)
            def _():
                for unit in units:
                    if unit[0]:
                        hop(*unit).wait_recv()
                        forward(unit)
                for place, (mask, half) in enumerate(units):
                    for w in range(hw):
                        base = (place * hw + w) * occ_p
                        if mask:
                            gz[base:base + occ, 0:orb] = slots[mask, half * hw + w]
                        else:
                            gz[base:base + occ, 0:orb] = greens_ref[half * hw + w]

        totals = [jnp.zeros((8, occ_p), jnp.float32) for _ in range(wl)]
        for t in range(tiles):
            both = jnp.dot(gz[...], lt[:, t * 2 * occ_p:(t + 1) * 2 * occ_p],
                           preferred_element_type=jnp.float32)
            for w in range(wl):
                first = both[w * occ_p:(w + 1) * occ_p, 0:occ_p]
                second = both[w * occ_p:(w + 1) * occ_p, occ_p:2 * occ_p]
                mixed = jnp.where(below, first, second)
                other = jnp.where(below, second, first)
                product = other * mixed.T
                totals[w] = totals[w] + jnp.sum(product.reshape(occ_p // 8, 8, occ_p), axis=0)
                dga[w, t:t + 1, :] = diagonal(first)
                dgb[w, t:t + 1, :] = diagonal(second)
        for w in range(wl):
            da = dga[w]
            db = dgb[w]
            gap = da - db
            ca = jnp.sum(da, axis=1, keepdims=True)
            cb = jnp.sum(db, axis=1, keepdims=True)
            coulomb = jnp.sum(0.5 * (ca * ca + cb * cb), axis=0, keepdims=True)
            row = -jnp.sum(totals[w], axis=0, keepdims=True) - 0.5 * jnp.sum(gap * gap, axis=0, keepdims=True)
            rows[pl.ds(s, 1), w:w + 1, :] = jnp.where(lane8[0:1] == 0, row + coulomb, row).reshape(1, 1, occ_p)
        return carry

    lax.fori_loop(0, len(steps), step_body, 0)

    for s, units in enumerate(steps):
        for place, (mask, half) in enumerate(units):
            at = flip(mask) * wl + half * hw
            for w in range(hw):
                part[pl.ds(at + w, 1), :] = rows[s, place * hw + w:place * hw + w + 1, :]

    width = box_x.shape[2]
    walkers = ngy * wl
    summed = jnp.sum(part[...], axis=1, keepdims=True)
    spot = (lax.broadcasted_iota(jnp.int32, (walkers, width), 0)
            == lax.broadcasted_iota(jnp.int32, (walkers, width), 1))
    line = jnp.sum(jnp.where(spot, summed, 0.0), axis=0, keepdims=True)
    msg_x[...] = jnp.broadcast_to(line, msg_x.shape)
    box_x[pl.ds(gx, 1)] = jnp.broadcast_to(line, msg_x.shape)[None]

    def x_copy(step):
        return pltpu.make_async_remote_copy(
            src_ref=msg_x, dst_ref=box_x.at[gx], send_sem=xs_sem.at[step - 1],
            recv_sem=xr_sem.at[step - 1], device_id=(x_peer(step), gy), device_id_type=MESH)

    for step in range(1, ngx):
        x_copy(step).start()

    lane_w = lax.broadcasted_iota(jnp.int32, (8, width), 1)
    sub_w = lax.broadcasted_iota(jnp.int32, (8, width), 0)
    extra = jnp.zeros((8, width), jnp.float32)
    for w in range(wl):
        single = jnp.sum(greens_ref[w].astype(jnp.float32) * body_ref[...], axis=0, keepdims=True)
        single = jnp.sum(single, axis=1, keepdims=True)
        mine = lane_w == gy * wl + w
        extra = extra + jnp.where(mine & (sub_w == 0), single, 0.0)
        extra = extra + jnp.where(mine & (sub_w == 1), weight_ref[0:1, w:w + 1], 0.0)

    for step in range(1, ngx):
        x_copy(step).wait_recv()
    total = jnp.sum(box_x[...], axis=0)
    message = jnp.where(sub_w == 0, total, 0.0) + extra
    msg_y[...] = message
    box_y[pl.ds(gy, 1)] = message[None]

    def y_copy(mask):
        return pltpu.make_async_remote_copy(
            src_ref=msg_y, dst_ref=box_y.at[gy], send_sem=ys_sem.at[mask - 1],
            recv_sem=yr_sem.at[mask - 1], device_id=(gx, flip(mask)), device_id_type=MESH)

    for mask in range(1, ngy):
        y_copy(mask).start()
    for mask in range(1, ngy):
        y_copy(mask).wait_recv()
    final = jnp.sum(box_y[...], axis=0)
    energy = final[0:1]
    weight = final[1:2]
    mean = (jnp.sum(energy * weight, axis=1, keepdims=True)
            / jnp.sum(weight, axis=1, keepdims=True))
    for w in range(wl):
        energy_ref[0:1, w:w + 1] = jnp.sum(
            jnp.where(lane_w[0:1] == gy * wl + w, energy, 0.0), axis=1, keepdims=True)
    mean_ref[...] = mean

    for step in range(1, ngx):
        x_copy(step).wait_send()
    for mask in range(1, ngy):
        y_copy(mask).wait_send()
        for half in range(halves):
            hop(mask, half).wait_send()


def shards(ngx, ngy, greens, chol_rot, one_body, weights):
    wl, occ, orb = greens.shape
    ng = chol_rot.shape[0]
    occ_p, orb_p = up(occ, LANE), up(orb, 2 * LANE)
    tiles = up(ng, 2) // 2
    halves = 2 if wl % 2 == 0 else 1
    width = up(ngy * wl, LANE)
    vmem = pl.BlockSpec(memory_space=pltpu.VMEM)
    f32, bf16 = jnp.float32, jnp.bfloat16
    dma = pltpu.SemaphoreType.DMA
    energy, mean = pl.pallas_call(
        functools.partial(kernel, ngx, ngy),
        out_shape=(jax.ShapeDtypeStruct((1, wl), f32), jax.ShapeDtypeStruct((1, 1), f32)),
        in_specs=[vmem] * 4,
        out_specs=(vmem, vmem),
        scratch_shapes=[
            pltpu.VMEM((ngy, wl, occ, orb), bf16),
            pltpu.VMEM((wl * occ_p, orb_p), bf16),
            pltpu.VMEM((occ_p, orb_p), bf16),
            pltpu.VMEM((orb_p, 2 * tiles * occ_p), bf16),
            pltpu.VMEM((wl, tiles, occ_p), f32),
            pltpu.VMEM((wl, tiles, occ_p), f32),
            pltpu.VMEM((ngy, wl, occ_p), f32),
            pltpu.VMEM((ngy * wl, occ_p), f32),
            pltpu.VMEM((ngx, 8, width), f32),
            pltpu.VMEM((ngy, 8, width), f32),
            pltpu.VMEM((8, width), f32),
            pltpu.VMEM((8, width), f32),
            dma((ngy, halves)), dma((ngy, halves)),
            dma((max(ngx - 1, 1),)), dma((max(ngx - 1, 1),)),
            dma((max(ngy - 1, 1),)), dma((max(ngy - 1, 1),)),
        ],
        compiler_params=pltpu.CompilerParams(
            collective_id=0, has_side_effects=True, vmem_limit_bytes=48 * 2**20),
    )(greens, chol_rot, one_body, weights.reshape(1, wl))
    return energy.reshape(wl), mean.reshape(())


def solution(mesh):
    ngx, ngy = mesh.shape["gx"], mesh.shape["gy"]
    placed = (P("gy", None, None), P(("gx", "gy"), None, None), P(), P("gy"))
    return jax.shard_map(
        functools.partial(shards, ngx, ngy), mesh=mesh, in_specs=placed,
        out_specs=(P("gy"), P()), check_vma=False,
    )
```

```python
import functools

import jax
import jax.numpy as jnp
from jax import lax
from jax.experimental import pallas as pl
from jax.experimental.pallas import tpu as pltpu
from jax.sharding import PartitionSpec as P

MESH = pl.DeviceIdType.MESH
LANE = 128


def up(value, unit):
    return -(-value // unit) * unit


def bits_of(mask):
    return [1 << b for b in range(mask.bit_length()) if mask >> b & 1]


def last_hop(mask, half):
    if mask & 1:
        return 1
    found = bits_of(mask)
    return found[-1] if half == 0 else found[0]


def depth_of(mask):
    return 2 * len(bits_of(mask & ~1)) + (mask & 1)


def arrival_steps(peers, halves):
    units = [(mask, half) for mask in range(peers) for half in range(halves)]
    if halves == 1:
        return [[unit] for unit in sorted(units, key=lambda u: (depth_of(u[0]), u[0]))]

    def rank(unit):
        mask, half = unit
        rest = mask & ~1
        late = 0
        if len(bits_of(rest)) == 1:
            late = (half + bits_of(rest)[0].bit_length()) % 2
        return (depth_of(mask), late, mask, half)

    units.sort(key=rank)
    return [units[i:i + 2] for i in range(0, len(units), 2)]


def kernel(ngx, ngy, greens_ref, chol_hbm, body_hbm, weight_hbm, energy_ref, mean_ref,
           chol_ref, body_ref, weight_ref, slots, gz, lp, lt, dga, dgb, rows, part, extra, box, msg,
           send_sem, recv_sem, load_sem, out_sem, in_sem):
    gx = lax.axis_index("gx")
    gy = lax.axis_index("gy")
    wl, occ, orb = greens_ref.shape
    ng = chol_ref.shape[0]
    occ_p = lp.shape[0]
    tiles = lt.shape[1] // (2 * occ_p)
    halves = 2 if wl % 2 == 0 else 1
    hw = wl // halves

    def flip(mask):
        there = gy
        for bit in bits_of(mask):
            there = there + bit * (1 - 2 * ((there // bit) % 2))
        return there

    def x_peer(step):
        return (gx + step) % ngx

    barrier = pltpu.get_barrier_semaphore()
    hops = [1 << b for b in range((ngy - 1).bit_length())]
    for mask in hops:
        pl.semaphore_signal(barrier, inc=1, device_id=(gx, flip(mask)), device_id_type=MESH)
    for step in range(1, ngx):
        pl.semaphore_signal(barrier, inc=1, device_id=(x_peer(step), gy), device_id_type=MESH)
    loads = [pltpu.make_async_copy(src, dst, load_sem.at[i]) for i, (src, dst) in enumerate(
        ((chol_hbm, chol_ref), (body_hbm, body_ref), (weight_hbm, weight_ref)))]
    for load in loads:
        load.start()
    pl.semaphore_wait(barrier, len(hops) + ngx - 1)

    def hop(mask, half):
        over = last_hop(mask, half)
        before = mask ^ over
        span = pl.ds(half * hw, hw)
        source = greens_ref.at[span] if before == 0 else slots.at[before, span]
        return pltpu.make_async_remote_copy(
            src_ref=source, dst_ref=slots.at[mask, span],
            send_sem=send_sem.at[mask, half], recv_sem=recv_sem.at[mask, half],
            device_id=(gx, flip(over)), device_id_type=MESH)

    steps = arrival_steps(ngy, halves)
    order = [unit for step in steps for unit in step]

    def forward(unit):
        for mask, half in order:
            if mask and half == unit[1] and mask ^ last_hop(mask, half) == unit[0]:
                hop(mask, half).start()

    for half in range(halves):
        forward((0, half))

    gz[...] = jnp.zeros_like(gz)
    lp[...] = jnp.zeros_like(lp)
    loads[0].wait()
    for g in range(2 * tiles):
        if g < ng:
            lp[0:occ, 0:orb] = chol_ref[g]
            lt[:, g * occ_p:(g + 1) * occ_p] = lp[...].T
        else:
            lt[:, g * occ_p:(g + 1) * occ_p] = jnp.zeros((lt.shape[0], occ_p), lt.dtype)

    loads[1].wait()
    loads[2].wait()
    lane_e = lax.broadcasted_iota(jnp.int32, extra.shape, 1)
    own = jnp.zeros(extra.shape, jnp.float32)
    for w in range(wl):
        single = jnp.sum(greens_ref[w].astype(jnp.float32) * body_ref[...], axis=0, keepdims=True)
        single = jnp.sum(single, axis=1, keepdims=True)
        own = own + jnp.where(lane_e == gy * wl + w, single, 0.0)
        own = own + jnp.where(lane_e == (ngy + gy) * wl + w, weight_ref[0:1, w:w + 1], 0.0)
    extra[...] = own

    lane8 = lax.broadcasted_iota(jnp.int32, (8, occ_p), 1)
    sub8 = lax.broadcasted_iota(jnp.int32, (8, occ_p), 0)
    on_diag = (lane8 % 8) == sub8
    below = (lax.broadcasted_iota(jnp.int32, (occ_p, occ_p), 0)
             > lax.broadcasted_iota(jnp.int32, (occ_p, occ_p), 1))

    def diagonal(block):
        picked = block[0:8]
        for k in range(1, occ_p // 8):
            picked = jnp.where(lane8 >= 8 * k, block[8 * k:8 * k + 8], picked)
        return jnp.sum(jnp.where(on_diag, picked, 0.0), axis=0, keepdims=True)

    def step_body(s, carry):
        for at, units in enumerate(steps):
            @pl.when(s == at)
            def _():
                for unit in units:
                    if unit[0]:
                        hop(*unit).wait_recv()
                        forward(unit)
                for place, (mask, half) in enumerate(units):
                    for w in range(hw):
                        base = (place * hw + w) * occ_p
                        if mask:
                            gz[base:base + occ, 0:orb] = slots[mask, half * hw + w]
                        else:
                            gz[base:base + occ, 0:orb] = greens_ref[half * hw + w]

        totals = [jnp.zeros((8, occ_p), jnp.float32) for _ in range(wl)]
        for t in range(tiles):
            both = jnp.dot(gz[...], lt[:, t * 2 * occ_p:(t + 1) * 2 * occ_p],
                           preferred_element_type=jnp.float32)
            for w in range(wl):
                first = both[w * occ_p:(w + 1) * occ_p, 0:occ_p]
                second = both[w * occ_p:(w + 1) * occ_p, occ_p:2 * occ_p]
                mixed = jnp.where(below, first, second)
                other = jnp.where(below, second, first)
                product = other * mixed.T
                totals[w] = totals[w] + jnp.sum(product.reshape(occ_p // 8, 8, occ_p), axis=0)
                dga[w, t:t + 1, :] = diagonal(first)
                dgb[w, t:t + 1, :] = diagonal(second)
        for w in range(wl):
            da = dga[w]
            db = dgb[w]
            gap = da - db
            ca = jnp.sum(da, axis=1, keepdims=True)
            cb = jnp.sum(db, axis=1, keepdims=True)
            coulomb = jnp.sum(0.5 * (ca * ca + cb * cb), axis=0, keepdims=True)
            row = -jnp.sum(totals[w], axis=0, keepdims=True) - 0.5 * jnp.sum(gap * gap, axis=0, keepdims=True)
            rows[pl.ds(s, 1), w:w + 1, :] = jnp.where(lane8[0:1] == 0, row + coulomb, row).reshape(1, 1, occ_p)
        return carry

    lax.fori_loop(0, len(steps), step_body, 0)

    for s, units in enumerate(steps):
        for place, (mask, half) in enumerate(units):
            at = flip(mask) * wl + half * hw
            for w in range(hw):
                part[pl.ds(at + w, 1), :] = rows[s, place * hw + w:place * hw + w + 1, :]

    width = box.shape[2]
    walkers = ngy * wl
    line = jnp.sum(part[...], axis=1, keepdims=True)
    row_at = lax.broadcasted_iota(jnp.int32, (walkers, width), 0)
    lane_at = lax.broadcasted_iota(jnp.int32, (walkers, width), 1)
    line = jnp.sum(jnp.where(row_at == lane_at, line, 0.0), axis=0, keepdims=True)
    line = line + jnp.where(gx == 0, extra[...], 0.0)
    msg[...] = line
    place = gx * ngy + gy
    box[pl.ds(place, 1)] = line[None]

    def share(across, mask):
        return pltpu.make_async_remote_copy(
            src_ref=msg, dst_ref=box.at[place], send_sem=out_sem.at[across, mask],
            recv_sem=in_sem.at[across, mask], device_id=(x_peer(across), flip(mask)),
            device_id_type=MESH)

    others = [(across, mask) for across in range(ngx) for mask in range(ngy) if across or mask]
    others.sort(key=lambda o: -(min(o[0], ngx - o[0]) + depth_of(o[1])))
    for other in others:
        share(*other).start()
    for other in others:
        share(*other).wait_recv()
    final = jnp.sum(box[...], axis=0)
    lane_1 = lane_at[0:1]
    weight = jnp.where(lane_1 >= walkers, final, 0.0)
    energy = jnp.where(lane_1 < walkers, final, 0.0)
    shifted = pltpu.roll(energy, walkers, 1)
    mean = (jnp.sum(shifted * weight, axis=1, keepdims=True)
            / jnp.sum(weight, axis=1, keepdims=True))
    for w in range(wl):
        energy_ref[0:1, w:w + 1] = jnp.sum(
            jnp.where(lane_1 == gy * wl + w, energy, 0.0), axis=1, keepdims=True)
    mean_ref[...] = mean

    for other in others:
        share(*other).wait_send()
    for mask in range(1, ngy):
        for half in range(halves):
            hop(mask, half).wait_send()


def shards(ngx, ngy, greens, chol_rot, one_body, weights):
    wl, occ, orb = greens.shape
    ng = chol_rot.shape[0]
    occ_p, orb_p = up(occ, LANE), up(orb, 2 * LANE)
    tiles = up(ng, 2) // 2
    halves = 2 if wl % 2 == 0 else 1
    width = up(2 * ngy * wl, LANE)
    vmem = pl.BlockSpec(memory_space=pltpu.VMEM)
    hbm = pl.BlockSpec(memory_space=pltpu.HBM)
    f32, bf16 = jnp.float32, jnp.bfloat16
    dma = pltpu.SemaphoreType.DMA
    energy, mean = pl.pallas_call(
        functools.partial(kernel, ngx, ngy),
        out_shape=(jax.ShapeDtypeStruct((1, wl), f32), jax.ShapeDtypeStruct((1, 1), f32)),
        in_specs=[vmem, hbm, hbm, hbm],
        out_specs=(vmem, vmem),
        scratch_shapes=[
            pltpu.VMEM((ng, occ, orb), bf16),
            pltpu.VMEM((occ, orb), f32),
            pltpu.VMEM((1, wl), f32),
            pltpu.VMEM((ngy, wl, occ, orb), bf16),
            pltpu.VMEM((wl * occ_p, orb_p), bf16),
            pltpu.VMEM((occ_p, orb_p), bf16),
            pltpu.VMEM((orb_p, 2 * tiles * occ_p), bf16),
            pltpu.VMEM((wl, tiles, occ_p), f32),
            pltpu.VMEM((wl, tiles, occ_p), f32),
            pltpu.VMEM((ngy, wl, occ_p), f32),
            pltpu.VMEM((ngy * wl, occ_p), f32),
            pltpu.VMEM((1, width), f32),
            pltpu.VMEM((ngx * ngy, 1, width), f32),
            pltpu.VMEM((1, width), f32),
            dma((ngy, halves)), dma((ngy, halves)),
            dma((3,)), dma((ngx, ngy)), dma((ngx, ngy)),
        ],
        compiler_params=pltpu.CompilerParams(
            collective_id=0, has_side_effects=True, vmem_limit_bytes=48 * 2**20),
    )(greens, chol_rot, one_body, weights.reshape(1, wl))
    return energy.reshape(wl), mean.reshape(())


def solution(mesh):
    ngx, ngy = mesh.shape["gx"], mesh.shape["gy"]
    placed = (P("gy", None, None), P(("gx", "gy"), None, None), P(), P("gy"))
    return jax.shard_map(
        functools.partial(shards, ngx, ngy), mesh=mesh, in_specs=placed,
        out_specs=(P("gy"), P()), check_vma=False,
    )
```

```python
import functools

import jax
import jax.numpy as jnp
from jax import lax
from jax.experimental import pallas as pl
from jax.experimental.pallas import tpu as pltpu
from jax.sharding import PartitionSpec as P

MESH = pl.DeviceIdType.MESH
LANE = 128


def up(value, unit):
    return -(-value // unit) * unit


def bits_of(mask):
    return [1 << b for b in range(mask.bit_length()) if mask >> b & 1]


def last_hop(mask, half):
    if mask & 1:
        return 1
    found = bits_of(mask)
    return found[-1] if half == 0 else found[0]


def depth_of(mask):
    return 2 * len(bits_of(mask & ~1)) + (mask & 1)


def arrival_steps(peers, halves):
    units = [(mask, half) for mask in range(peers) for half in range(halves)]
    if halves == 1:
        return [[unit] for unit in sorted(units, key=lambda u: (depth_of(u[0]), u[0]))]

    def rank(unit):
        mask, half = unit
        rest = mask & ~1
        late = 0
        if len(bits_of(rest)) == 1:
            late = (half + bits_of(rest)[0].bit_length()) % 2
        return (len(bits_of(rest)), late, mask & 1, mask, half)

    units.sort(key=rank)
    return [units[i:i + 2] for i in range(0, len(units), 2)]


def kernel(ngx, ngy, greens_ref, chol_hbm, body_hbm, weight_hbm, energy_ref, mean_ref,
           chol_ref, body_ref, weight_ref, slots, gz, lp, lt, dga, dgb, rows, part, extra, box, msg,
           send_sem, recv_sem, load_sem, out_sem, in_sem):
    gx = lax.axis_index("gx")
    gy = lax.axis_index("gy")
    wl, occ, orb = greens_ref.shape
    ng = chol_ref.shape[0]
    occ_p = lp.shape[0]
    tiles = lt.shape[1] // (2 * occ_p)
    halves = 2 if wl % 2 == 0 else 1
    hw = wl // halves

    def flip(mask):
        there = gy
        for bit in bits_of(mask):
            there = there + bit * (1 - 2 * ((there // bit) % 2))
        return there

    def x_peer(step):
        return (gx + step) % ngx

    barrier = pltpu.get_barrier_semaphore()
    hops = [1 << b for b in range((ngy - 1).bit_length())]
    for mask in hops:
        pl.semaphore_signal(barrier, inc=1, device_id=(gx, flip(mask)), device_id_type=MESH)
    for step in range(1, ngx):
        pl.semaphore_signal(barrier, inc=1, device_id=(x_peer(step), gy), device_id_type=MESH)
    loads = [pltpu.make_async_copy(src, dst, load_sem.at[i]) for i, (src, dst) in enumerate(
        ((chol_hbm, chol_ref), (body_hbm, body_ref), (weight_hbm, weight_ref)))]
    for load in loads:
        load.start()
    pl.semaphore_wait(barrier, len(hops) + ngx - 1)

    def hop(mask, half):
        over = last_hop(mask, half)
        before = mask ^ over
        span = pl.ds(half * hw, hw)
        source = greens_ref.at[span] if before == 0 else slots.at[before, span]
        return pltpu.make_async_remote_copy(
            src_ref=source, dst_ref=slots.at[mask, span],
            send_sem=send_sem.at[mask, half], recv_sem=recv_sem.at[mask, half],
            device_id=(gx, flip(over)), device_id_type=MESH)

    steps = arrival_steps(ngy, halves)
    order = [unit for step in steps for unit in step]

    def forward(unit):
        for mask, half in order:
            if mask and half == unit[1] and mask ^ last_hop(mask, half) == unit[0]:
                hop(mask, half).start()

    for mask, half in order:
        if mask and mask == last_hop(mask, half):
            hop(mask, half).start()

    gz[...] = jnp.zeros_like(gz)
    lp[...] = jnp.zeros_like(lp)
    loads[0].wait()
    for g in range(2 * tiles):
        if g < ng:
            lp[0:occ, 0:orb] = chol_ref[g]
            lt[:, g * occ_p:(g + 1) * occ_p] = lp[...].T
        else:
            lt[:, g * occ_p:(g + 1) * occ_p] = jnp.zeros((lt.shape[0], occ_p), lt.dtype)

    loads[1].wait()
    loads[2].wait()
    lane_e = lax.broadcasted_iota(jnp.int32, extra.shape, 1)
    own = jnp.zeros(extra.shape, jnp.float32)
    for w in range(wl):
        single = jnp.sum(greens_ref[w].astype(jnp.float32) * body_ref[...], axis=0, keepdims=True)
        single = jnp.sum(single, axis=1, keepdims=True)
        own = own + jnp.where(lane_e == gy * wl + w, single, 0.0)
        own = own + jnp.where(lane_e == (ngy + gy) * wl + w, weight_ref[0:1, w:w + 1], 0.0)
    extra[...] = own

    lane8 = lax.broadcasted_iota(jnp.int32, (8, occ_p), 1)
    sub8 = lax.broadcasted_iota(jnp.int32, (8, occ_p), 0)
    on_diag = (lane8 % 8) == sub8
    below = (lax.broadcasted_iota(jnp.int32, (occ_p, occ_p), 0)
             > lax.broadcasted_iota(jnp.int32, (occ_p, occ_p), 1))

    def diagonal(block):
        picked = block[0:8]
        for k in range(1, occ_p // 8):
            picked = jnp.where(lane8 >= 8 * k, block[8 * k:8 * k + 8], picked)
        return jnp.sum(jnp.where(on_diag, picked, 0.0), axis=0, keepdims=True)

    def step_body(s, carry):
        for at, units in enumerate(steps):
            @pl.when(s == at)
            def _():
                for unit in units:
                    if unit[0]:
                        hop(*unit).wait_recv()
                        forward(unit)
                for place, (mask, half) in enumerate(units):
                    for w in range(hw):
                        base = (place * hw + w) * occ_p
                        if mask:
                            gz[base:base + occ, 0:orb] = slots[mask, half * hw + w]
                        else:
                            gz[base:base + occ, 0:orb] = greens_ref[half * hw + w]

        totals = [jnp.zeros((8, occ_p), jnp.float32) for _ in range(wl)]
        for t in range(tiles):
            both = jnp.dot(gz[...], lt[:, t * 2 * occ_p:(t + 1) * 2 * occ_p],
                           preferred_element_type=jnp.float32)
            for w in range(wl):
                first = both[w * occ_p:(w + 1) * occ_p, 0:occ_p]
                second = both[w * occ_p:(w + 1) * occ_p, occ_p:2 * occ_p]
                mixed = jnp.where(below, first, second)
                other = jnp.where(below, second, first)
                product = other * mixed.T
                totals[w] = totals[w] + jnp.sum(product.reshape(occ_p // 8, 8, occ_p), axis=0)
                dga[w, t:t + 1, :] = diagonal(first)
                dgb[w, t:t + 1, :] = diagonal(second)
        for w in range(wl):
            da = dga[w]
            db = dgb[w]
            gap = da - db
            ca = jnp.sum(da, axis=1, keepdims=True)
            cb = jnp.sum(db, axis=1, keepdims=True)
            coulomb = jnp.sum(0.5 * (ca * ca + cb * cb), axis=0, keepdims=True)
            row = -jnp.sum(totals[w], axis=0, keepdims=True) - 0.5 * jnp.sum(gap * gap, axis=0, keepdims=True)
            rows[pl.ds(s, 1), w:w + 1, :] = jnp.where(lane8[0:1] == 0, row + coulomb, row).reshape(1, 1, occ_p)
        return carry

    lax.fori_loop(0, len(steps), step_body, 0)

    for s, units in enumerate(steps):
        for place, (mask, half) in enumerate(units):
            at = flip(mask) * wl + half * hw
            for w in range(hw):
                part[pl.ds(at + w, 1), :] = rows[s, place * hw + w:place * hw + w + 1, :]

    width = box.shape[2]
    walkers = ngy * wl
    line = jnp.sum(part[...], axis=1, keepdims=True)
    row_at = lax.broadcasted_iota(jnp.int32, (walkers, width), 0)
    lane_at = lax.broadcasted_iota(jnp.int32, (walkers, width), 1)
    line = jnp.sum(jnp.where(row_at == lane_at, line, 0.0), axis=0, keepdims=True)
    line = line + jnp.where(gx == 0, extra[...], 0.0)
    msg[...] = line
    place = gx * ngy + gy
    box[pl.ds(place, 1)] = line[None]

    def share(across, mask):
        return pltpu.make_async_remote_copy(
            src_ref=msg, dst_ref=box.at[place], send_sem=out_sem.at[across, mask],
            recv_sem=in_sem.at[across, mask], device_id=(x_peer(across), flip(mask)),
            device_id_type=MESH)

    others = [(across, mask) for across in range(ngx) for mask in range(ngy) if across or mask]
    others.sort(key=lambda o: -(min(o[0], ngx - o[0]) + depth_of(o[1])))
    for other in others:
        share(*other).start()
    for other in others:
        share(*other).wait_recv()
    final = jnp.sum(box[...], axis=0)
    lane_1 = lane_at[0:1]
    weight = jnp.where(lane_1 >= walkers, final, 0.0)
    energy = jnp.where(lane_1 < walkers, final, 0.0)
    shifted = pltpu.roll(energy, walkers, 1)
    mean = (jnp.sum(shifted * weight, axis=1, keepdims=True)
            / jnp.sum(weight, axis=1, keepdims=True))
    for w in range(wl):
        energy_ref[0:1, w:w + 1] = jnp.sum(
            jnp.where(lane_1 == gy * wl + w, energy, 0.0), axis=1, keepdims=True)
    mean_ref[...] = mean

    for other in others:
        share(*other).wait_send()
    for mask in range(1, ngy):
        for half in range(halves):
            hop(mask, half).wait_send()


def shards(ngx, ngy, greens, chol_rot, one_body, weights):
    wl, occ, orb = greens.shape
    ng = chol_rot.shape[0]
    occ_p, orb_p = up(occ, LANE), up(orb, 2 * LANE)
    tiles = up(ng, 2) // 2
    halves = 2 if wl % 2 == 0 else 1
    width = up(2 * ngy * wl, LANE)
    vmem = pl.BlockSpec(memory_space=pltpu.VMEM)
    hbm = pl.BlockSpec(memory_space=pltpu.HBM)
    f32, bf16 = jnp.float32, jnp.bfloat16
    dma = pltpu.SemaphoreType.DMA
    energy, mean = pl.pallas_call(
        functools.partial(kernel, ngx, ngy),
        out_shape=(jax.ShapeDtypeStruct((1, wl), f32), jax.ShapeDtypeStruct((1, 1), f32)),
        in_specs=[vmem, hbm, hbm, hbm],
        out_specs=(vmem, vmem),
        scratch_shapes=[
            pltpu.VMEM((ng, occ, orb), bf16),
            pltpu.VMEM((occ, orb), f32),
            pltpu.VMEM((1, wl), f32),
            pltpu.VMEM((ngy, wl, occ, orb), bf16),
            pltpu.VMEM((wl * occ_p, orb_p), bf16),
            pltpu.VMEM((occ_p, orb_p), bf16),
            pltpu.VMEM((orb_p, 2 * tiles * occ_p), bf16),
            pltpu.VMEM((wl, tiles, occ_p), f32),
            pltpu.VMEM((wl, tiles, occ_p), f32),
            pltpu.VMEM((ngy, wl, occ_p), f32),
            pltpu.VMEM((ngy * wl, occ_p), f32),
            pltpu.VMEM((1, width), f32),
            pltpu.VMEM((ngx * ngy, 1, width), f32),
            pltpu.VMEM((1, width), f32),
            dma((ngy, halves)), dma((ngy, halves)),
            dma((3,)), dma((ngx, ngy)), dma((ngx, ngy)),
        ],
        compiler_params=pltpu.CompilerParams(
            collective_id=0, has_side_effects=True, vmem_limit_bytes=63 * 2**20),
    )(greens, chol_rot, one_body, weights.reshape(1, wl))
    return energy.reshape(wl), mean.reshape(())


def solution(mesh):
    ngx, ngy = mesh.shape["gx"], mesh.shape["gy"]
    placed = (P("gy", None, None), P(("gx", "gy"), None, None), P(), P("gy"))
    return jax.shard_map(
        functools.partial(shards, ngx, ngy), mesh=mesh, in_specs=placed,
        out_specs=(P("gy"), P()), check_vma=False,
    )
```
